32 devices in a mesh: dp: 8 (over z, y), group: 4 (over x, core).
Axes of the slice: x: 2, y: 2, z: 4, core: 2. Of those that a mesh axis runs over, the one named last changes fastest.
Arguments:
- keys: int32 [16384], P(('dp', 'group')), may hold values from 0 to 1073741823
- cut: int32 [1], replicated, may hold values from 256 to 1023
- owner: int32 [16384, 1], P(('dp', 'group')), may hold values from 0 to 7; in each aligned block of 512 rows (0 to 511, 512 to 1023, ...) at most 128 rows name the same one
- tokens: int32 [16384, 2048], P(('dp', 'group')), may hold values from 0 to 128255
Outputs:
- histogram: int32 [4096], replicated
- packed_rows: int32 [32768, 2048], P(('dp', 'group'))
- packed_weights: float32 [32768], P(('dp', 'group'))
The draws below stay inside these ranges and needn't reach their ends.
Inputs may be any that keep to these rules, and one draw needn't show every extreme that they name: Among the examples of one device, at most 128 have the same owner, and some owner has exactly 128.
All inputs are finite; a program needn't handle non-finite values.
Results may differ from the reference program's by a relative error of at most 0.0003.
Values sent between devices are 32-bit elements; how exact they have to be, the bound alone decides.
A program may use at most 128 MiB of HBM per device.

```python
import math
import jax
import jax.numpy as jnp
import numpy as np

EX_DEV = 512
SEQ = 2048
BINS = 4096
BIN_WIDTH = 262144
VOCAB = 128256
EXAMPLES = 16384
MOST = 128
RECV = 1024
N_DP = 8
N_GROUP = 4


def place_ends(array, rng, smallest, top_value):
    extent = array.shape
    place = [jax.random.randint(jax.random.fold_in(rng, axis), (), 0, extent[axis]) for axis in range(len(extent))]
    array = array.at[tuple(place)].set(smallest)
    longest = extent.index(max(extent))
    place[longest] = (place[longest] + 1) % extent[longest]
    return array.at[tuple(place)].set(top_value)


def ranked_wide(rng, extent, amount, slope):
    weights = [min(1 << octave, amount + 1 - (1 << octave)) * (1 << 20) // math.isqrt((1 << octave) ** slope) + 1 for octave in range((amount + 1).bit_length()) if 1 << octave <= amount]
    scale = 1 + sum(weights) // (1 << 30)
    table = np.cumsum(np.array([max(1, weight // scale) for weight in weights]))
    ticket = jax.random.randint(jax.random.fold_in(rng, 1), extent, 0, int(table[len(weights) - 1]))
    start = jnp.left_shift(1, jnp.searchsorted(jnp.asarray(table, jnp.int32), ticket, side="right").astype(jnp.int32))
    rank = start - 1 + jax.random.randint(jax.random.fold_in(rng, 4), extent, 0, 1 << 30) % jnp.minimum(start, amount + 1 - start)
    return jax.random.permutation(jax.random.fold_in(rng, 2), amount)[rank].astype(jnp.int32)


def deal_out(rng, own, number, rows, number_of, top, limit, slope):
    ranking = jax.random.permutation(rng, number_of)
    packed, common = shares(number_of, rows * top, limit, slope, True), shares(number_of, rows * top, limit, slope, False)
    places = jnp.arange(number_of)

    def named(sizes, rotation):
        used = int((sizes > 0).sum())
        fixed = max(1, used // 4)
        moved = fixed + (places - fixed + rotation * (used - fixed)) % max(1, number_of - fixed)
        return jnp.zeros((number_of,), jnp.int32).at[ranking[jnp.where(places < fixed, places, moved)]].set(jnp.asarray(sizes, jnp.int32))

    sizes = jnp.where(number % 4 == 0, named(packed, number // 4), named(common, number - number // 4 - 1))
    mixed = jax.random.permutation(jax.random.fold_in(own, 3), number_of)
    donor, taker = mixed[0:number_of // 2 * 2:2], mixed[1:number_of // 2 * 2:2]
    margin = jnp.minimum(sizes[donor] - 1, limit - sizes[taker]) // 2
    margin = jnp.where((donor == ranking[0]) | (taker == ranking[0]) | (sizes[taker] == 0), 0, jnp.maximum(margin, 0))
    moved = jax.random.randint(jax.random.fold_in(own, 4), (number_of // 2,), 0, 1 << 20) % (margin + 1)
    sizes = sizes.at[donor].add(-moved).at[taker].add(moved)
    members = jnp.searchsorted(jnp.cumsum(sizes), jnp.arange(rows * top), side="right").astype(jnp.int32)
    table = members.reshape(top, rows).T
    table = table[jax.random.permutation(jax.random.fold_in(own, 1), rows)]
    rotation = jax.random.randint(jax.random.fold_in(own, 2), (rows, 1), 0, top)
    return jnp.take_along_axis(table, (jnp.arange(top)[None, :] + rotation) % top, axis=1)


def shares(count, total, bound, slope, full):
    weights = [(1 << 20) // math.isqrt(standing ** slope) + 1 for standing in range(1, count + 1)]
    largest = bound if full else min(bound, max(-(-total // count), total * weights[0] // sum(weights)))
    least = 1 if total - largest >= count - 1 else 0
    counts, spare = [largest] + [least] * (count - 1), total - largest - least * (count - 1)
    while spare > 0:
        free = [i for i in range(1, count) if counts[i] < largest] or [i for i in range(1, count) if counts[i] < bound]
        mass, remaining = sum([weights[i] for i in free]), spare
        for i in free:
            more = min(bound - counts[i], max(1, remaining * weights[i] // mass), spare)
            counts[i] = counts[i] + more
            spare = spare - more
    return np.array(counts)


def setup_inputs(seed: int = 0) -> dict:
    splits = jax.random.split(jax.random.key(seed), 5)
    keys = place_ends(jax.random.randint(splits[0], (EXAMPLES,), 0, BINS * BIN_WIDTH), jax.random.fold_in(splits[0], 1), 0, (BINS * BIN_WIDTH) - 1).astype(jnp.int32)
    cut = jax.random.randint(splits[1], (1,), BINS // 16, BINS // 4).astype(jnp.int32)
    owner_keys = jax.random.split(jax.random.fold_in(splits[2], 1), EXAMPLES // EX_DEV)
    owner_turns = jax.random.permutation(jax.random.fold_in(splits[2], 3), EXAMPLES // EX_DEV)
    owner = jax.vmap(lambda own, number: deal_out(jax.random.fold_in(splits[2], 2), own, number, EX_DEV, N_DP, 1, MOST, 2))(owner_keys, owner_turns).reshape((EXAMPLES, 1))
    tokens = place_ends(ranked_wide(splits[3], (EXAMPLES, SEQ), VOCAB, 2), jax.random.fold_in(splits[3], 3), 0, VOCAB - 1).astype(jnp.int32)
    return {"keys": keys, "cut": cut, "owner": owner, "tokens": tokens}


def reference(keys, cut, owner, tokens):
    bins_of = keys // BIN_WIDTH
    hist = jnp.zeros((BINS,), jnp.float32).at[bins_of].add(1.0)
    kept = bins_of >= cut[0]
    dest = owner[:, 0]
    onehot = ((dest[:, None] == jnp.arange(N_DP, dtype=jnp.int32)[None, :]) & kept[:, None]).astype(jnp.int32)
    running = jnp.cumsum(onehot, axis=0) - onehot
    rank = jnp.sum(running * onehot, axis=1)
    device = dest * N_GROUP + rank % N_GROUP
    slot = rank // N_GROUP
    count = N_DP * N_GROUP * RECV
    target = jnp.where(kept, device * RECV + slot, count).astype(jnp.int32)
    suffix = jnp.cumsum(hist[::-1])[::-1]
    total = jnp.maximum(suffix[cut[0]], 1.0)
    weight = suffix[bins_of] / total
    packed_rows = jnp.zeros((count, SEQ), jnp.int32).at[target].set(tokens, mode="drop")
    packed_weights = jnp.zeros((count,), jnp.float32).at[target].set(weight, mode="drop")
    return hist.astype(jnp.int32), packed_rows, packed_weights
```

```python
import functools
import itertools

import jax
import jax.numpy as jnp
import numpy as np
from jax import lax
from jax.experimental import pallas as pl
from jax.experimental.pallas import tpu as pltpu
from jax.sharding import PartitionSpec as P

BINS = 4096
BIN_WIDTH = 262144
LANES = 128
LEVELS = ((28, 18), (31, 20))
MESH = pl.DeviceIdType.MESH


def peer(me, i, n):
    off = i + n // 2
    off = off - lax.div(off, n) * (n - 1)
    return lax.rem(me + off, n)


def place(d, n_member):
    return (lax.div(d, n_member), lax.rem(d, n_member))


def greet(me, n, n_member):
    barrier = pltpu.get_barrier_semaphore()

    def signal(i, c):
        pl.semaphore_signal(
            barrier, inc=1, device_id=place(peer(me, i, n), n_member), device_id_type=MESH
        )
        return c

    lax.fori_loop(0, n - 1, signal, 0)


def met(n):
    pl.semaphore_wait(pltpu.get_barrier_semaphore(), n - 1)


def meta_kernel(n, n_member, mine, every, local_sem, send_sem, recv_sem):
    me = lax.axis_index("dp") * n_member + lax.axis_index("group")
    own = pltpu.make_async_copy(mine, every.at[me], local_sem)
    own.start()
    greet(me, n, n_member)
    met(n)

    def start(i, c):
        d = peer(me, i, n)
        pltpu.make_async_remote_copy(
            src_ref=mine,
            dst_ref=every.at[me],
            send_sem=send_sem,
            recv_sem=recv_sem,
            device_id=place(d, n_member),
            device_id_type=MESH,
        ).start()
        return c

    lax.fori_loop(0, n - 1, start, 0)
    own.wait()
    rest = every.at[pl.ds(0, n - 1)]
    for sem in (send_sem, recv_sem):
        pltpu.make_async_copy(rest, rest, sem).wait()


def rows_kernel(
    n, n_member, slots, wide, w, narrow, w1, caps, pieces,
    index, spill_index, cut, tokens, keys_all, owner_all,
    got, hist, weights,
    held, send, leaving, joined, spot, table, tail,
    load_sem, own_sem, send_sem, recv_sem, leave_sem, join_sem,
):
    me_dp, me_group = lax.axis_index("dp"), lax.axis_index("group")
    me = me_dp * n_member + me_group
    spill = narrow < slots
    examples = held.shape[0]
    for p in range(pieces):
        pltpu.make_async_copy(
            tokens.at[:, pl.ds(p * LANES, LANES)], held.at[:, p, :], load_sem
        ).start()
    greet(me, n, n_member)
    pltpu.make_async_copy(got.at[pl.ds(0, examples)], held, load_sem).wait()

    def is_wide(d):
        at = lax.div(d, n_member)
        found = at == wide[0]
        for o in wide[1:]:
            found = jnp.logical_or(found, at == o)
        return found

    def fill1(d):
        for j in range(w1):
            send[d * w + j] = held[index[d * slots + j]]

    def fill2(d, first, last):
        def one(j, c):
            at = index[d * slots + j]
            if spill:
                local = held[jnp.minimum(at, examples - 1)]
                moved = joined[jnp.maximum(at - examples, 0)]
                send[d * w + j] = jnp.where(at < examples, local, moved)
            else:
                send[d * w + j] = held[at]
            return c

        lax.fori_loop(first, last, one, 0)

    def remote(src, dst, out_sem, in_sem, d):
        return pltpu.make_async_remote_copy(
            src_ref=src, dst_ref=dst, send_sem=out_sem, recv_sem=in_sem,
            device_id=place(d, n_member), device_id_type=MESH,
        )

    def part1(d, at):
        return remote(
            send.at[pl.ds(d * w, w1)], got.at[pl.ds(at * w1, w1)], send_sem, recv_sem, d
        )

    def part2(d, at):
        return remote(
            send.at[pl.ds(d * w + w1, narrow - w1)],
            got.at[pl.ds(n * w1 + at * (w - w1), narrow - w1)], send_sem, recv_sem, d,
        )

    def part3(d, at):
        return remote(
            send.at[pl.ds(d * w + narrow, w - narrow)],
            got.at[pl.ds(n * w1 + at * (w - w1) + narrow - w1, w - narrow)],
            send_sem, recv_sem, d,
        )

    def when_wide(d, act):
        if wide:
            pl.when(is_wide(d))(act)

    moves = []
    if spill:
        base = me_group - lax.rem(me_group, 4)
        mine = me_group - base
        core, column = lax.rem(mine, 2), lax.div(mine, 2)
        begin = 0
        for k, cap in enumerate(caps):
            other = base + (column if k == 0 else 1 - column) * 2 + (core if k == 1 else 1 - core)
            rows = pl.ds(begin, cap)
            moves.append(
                remote(
                    leaving.at[rows], joined.at[rows], leave_sem, join_sem,
                    me_dp * n_member + other,
                )
            )
            begin += cap

        def leave(g, c):
            for j in range(4):
                at = g * 4 + j
                leaving[at] = held[spill_index[at]]
            return c

        lax.fori_loop(0, begin // 4, leave, 0)
    met(n)
    for move in moves:
        move.start()

    def start1(i, c):
        d = peer(me, i, n)
        fill1(d)
        part1(d, me).start()
        return c

    lax.fori_loop(0, n - 1, start1, 0)
    if spill:
        everything = pl.ds(0, sum(caps))
        pltpu.make_async_copy(leaving.at[everything], joined.at[everything], join_sem).wait()

    def start2(i, c):
        d = peer(me, i, n)
        fill2(d, w1, narrow)
        part2(d, me).start()

        def rest():
            fill2(d, narrow, w)
            part3(d, me).start()

        when_wide(d, rest)
        return c

    lax.fori_loop(0, n - 1, start2, 0)
    fill1(me)
    fill2(me, w1, w)
    owns = [
        pltpu.make_async_copy(
            send.at[pl.ds(me * w, w1)], got.at[pl.ds(me * w1, w1)], own_sem
        ),
        pltpu.make_async_copy(
            send.at[pl.ds(me * w + w1, w - w1)],
            got.at[pl.ds(n * w1 + me * (w - w1), w - w1)], own_sem,
        ),
    ]
    for own in owns:
        own.start()

    hist[...] = jnp.zeros_like(hist)
    tail[...] = jnp.zeros_like(tail)
    hi_of = lax.broadcasted_iota(jnp.int32, (BINS // LANES, LANES), 0)
    lo_of = lax.broadcasted_iota(jnp.int32, (LANES, LANES), 0)
    row_of = lax.broadcasted_iota(jnp.int32, (LANES, LANES), 0)
    lane_of = lax.broadcasted_iota(jnp.int32, (LANES, LANES), 1)
    earlier = jnp.where(row_of < lane_of, 1.0, 0.0).astype(jnp.bfloat16)
    ones = jnp.ones((LANES, LANES), jnp.bfloat16)

    def count(r, seen):
        bins = keys_all[pl.ds(r, 1), :] // BIN_WIDTH
        hi = jnp.where(hi_of == bins // LANES, 1.0, 0.0).astype(jnp.bfloat16)
        lo = jnp.where(lo_of == bins % LANES, 1.0, 0.0).astype(jnp.bfloat16)
        hist[...] += lax.dot_general(
            hi, lo, (((1,), (1,)), ((), ())), preferred_element_type=jnp.float32
        )
        above = jnp.where(hi_of < bins // LANES, 1.0, 0.0).astype(jnp.bfloat16)
        reach = jnp.where(lo_of <= bins % LANES, 1.0, 0.0).astype(jnp.bfloat16)
        tail[...] += lax.dot_general(
            hi, reach, (((1,), (1,)), ((), ())), preferred_element_type=jnp.float32
        ) + lax.dot_general(
            above, ones, (((1,), (0,)), ((), ())), preferred_element_type=jnp.float32
        )
        mine = jnp.logical_and(owner_all[pl.ds(r, 1), :] == me_dp, bins >= cut[0])
        flags = jnp.where(mine, 1.0, 0.0)
        eight = jnp.broadcast_to(flags, (8, LANES)).astype(jnp.bfloat16)
        below = lax.dot_general(
            eight, earlier, (((1,), (0,)), ((), ())), preferred_element_type=jnp.float32
        )[0:1]
        whole = lax.dot_general(
            eight, ones, (((1,), (0,)), ((), ())), preferred_element_type=jnp.float32
        )[0:1]
        rank = (below + seen).astype(jnp.int32)
        here = jnp.logical_and(mine, rank % n_member == me_group)
        spot[pl.ds(r, 1), :] = jnp.where(here, rank // n_member, -1)
        return seen + whole

    lax.fori_loop(0, keys_all.shape[0], count, jnp.zeros((1, LANES), jnp.float32))

    suffix = tail[...]
    upper = jnp.floor(suffix * (1.0 / LANES))
    table[...] = jnp.concatenate([upper, suffix - upper * LANES], axis=0).astype(jnp.bfloat16)
    bin_of = hi_of * LANES + lax.broadcasted_iota(jnp.int32, hi_of.shape, 1)
    kept = jnp.sum(
        jnp.sum(jnp.where(bin_of == cut[0], suffix, 0.0), axis=1, keepdims=True),
        axis=0, keepdims=True,
    )
    total = jnp.maximum(kept, 1.0)
    groups = weights.shape[0]
    group_of = lax.broadcasted_iota(jnp.int32, (groups, LANES), 0)
    weights[...] = jnp.zeros_like(weights)

    def weigh(r, c):
        bins = keys_all[pl.ds(r, 1), :] // BIN_WIDTH
        slot = spot[pl.ds(r, 1), :]
        lo = jnp.where(lo_of == bins % LANES, 1.0, 0.0).astype(jnp.bfloat16)
        rows = lax.dot_general(
            table[...], lo, (((1,), (0,)), ((), ())), preferred_element_type=jnp.float32
        )
        pick = hi_of == bins // LANES
        up = jnp.sum(jnp.where(pick, rows[: BINS // LANES], 0.0), axis=0, keepdims=True)
        down = jnp.sum(jnp.where(pick, rows[BINS // LANES :], 0.0), axis=0, keepdims=True)
        at = jnp.logical_and(slot >= 0, group_of == slot // LANES)
        column = jnp.where(lo_of == slot % LANES, 1.0, 0.0).astype(jnp.bfloat16)
        both = jnp.concatenate([jnp.where(at, up, 0.0), jnp.where(at, down, 0.0)], axis=0)
        laid = lax.dot_general(
            both.astype(jnp.bfloat16), column, (((1,), (1,)), ((), ())),
            preferred_element_type=jnp.float32,
        )
        weights[...] += laid[:groups] * LANES + laid[groups:]
        return c

    lax.fori_loop(0, keys_all.shape[0], weigh, 0)
    weights[...] = weights[...] / total

    def done(rows, sem):
        rows = pl.ds(0, rows)
        pltpu.make_async_copy(send.at[rows], got.at[rows], sem).wait()

    done(w, own_sem)
    if spill:
        pltpu.make_async_copy(leaving.at[everything], joined.at[everything], leave_sem).wait()
    out = (n - len(wide) * n_member) * narrow + len(wide) * n_member * w
    if wide:
        def ends(size):
            done(out - size, send_sem)
            done((n - 1) * size, recv_sem)

        pl.when(is_wide(me))(functools.partial(ends, w))
        pl.when(jnp.logical_not(is_wide(me)))(functools.partial(ends, narrow))
    else:
        done(out - w, send_sem)
        done((n - 1) * w, recv_sem)


def pack_kernel(pieces, chunk, index, got, out, held, made, load_sem, out_sem):
    rows = got.shape[0]
    slots = made.shape[0]
    load = pltpu.make_async_copy(got, held.at[pl.ds(0, rows)], load_sem)
    load.start()
    held[rows] = jnp.zeros(held.shape[1:], jnp.int32)
    load.wait()

    def stores(k):
        return [
            pltpu.make_async_copy(
                made.at[pl.ds(k * chunk, chunk), p, :],
                out.at[pl.ds(k * chunk, chunk), pl.ds(p * LANES, LANES)],
                out_sem.at[k, p],
            )
            for p in range(pieces)
        ]

    def fill(k):
        def some(g, c):
            for j in range(8):
                s = k * chunk + g * 8 + j
                made[s] = held[index[s]]
            return c

        lax.fori_loop(0, chunk // 8, some, 0)

    def step(k, c):
        fill(k)
        for copy in stores(k):
            copy.start()
        return c

    def finish(k, c):
        for copy in stores(k):
            copy.wait()
        return c

    lax.fori_loop(0, slots // chunk, step, 0)
    lax.fori_loop(0, slots // chunk, finish, 0)


def flows(views, w, w1):
    over = [jnp.maximum(v - w, 0) for v in views]
    free = [w - jnp.maximum(jnp.minimum(v, w), w1) for v in views]
    moved = []
    for step in (1, 2, 3):
        flow = [jnp.minimum(over[k], free[k ^ step]) for k in range(4)]
        over = [over[k] - flow[k] for k in range(4)]
        free = [free[k] - flow[k ^ step] for k in range(4)]
        moved.append(flow)
    return over[0], moved


def body(n_owner, n_member, keys, cut, owner, tokens):
    examples, width = tokens.shape
    n = n_owner * n_member
    slots = 2 * examples // n
    capacity = 2 * examples
    pieces = width // LANES
    per = examples // LANES
    me_dp, me_group = lax.axis_index("dp"), lax.axis_index("group")
    me = me_dp * n_member + me_group
    vmem = pl.BlockSpec(memory_space=pltpu.VMEM)
    smem = pl.BlockSpec(memory_space=pltpu.SMEM)
    hbm = pl.BlockSpec(memory_space=pl.ANY)
    dest = owner[:, 0]
    i32 = jnp.int32

    mine = jnp.concatenate([keys.reshape(per, LANES), dest.reshape(per, LANES)], axis=0)
    every = pl.pallas_call(
        functools.partial(meta_kernel, n, n_member),
        out_shape=jax.ShapeDtypeStruct((n, 2 * per, LANES), jnp.int32),
        in_specs=[vmem],
        out_specs=vmem,
        scratch_shapes=[
            pltpu.SemaphoreType.DMA,
            pltpu.SemaphoreType.DMA,
            pltpu.SemaphoreType.DMA,
        ],
        compiler_params=pltpu.CompilerParams(collective_id=0, has_side_effects=True),
    )(mine)
    keys_all = every[:, :per].reshape(n * per, LANES)
    owner_all = every[:, per:].reshape(n * per, LANES)
    code_all = jnp.where(keys_all // BIN_WIDTH >= cut[0], owner_all, -1).reshape(n, examples)
    owners = jnp.arange(n_owner, dtype=i32)
    table = jnp.sum(code_all[:, None, :] == owners[None, :, None], axis=2, dtype=i32)
    source = jnp.arange(n, dtype=i32)
    before = jnp.sum(
        jnp.where((source[None, :] < source[:, None])[:, :, None], table[None], 0), axis=1
    )

    lane = np.arange(n)
    spread = (lane[None, :] // n_member == np.arange(n_owner)[:, None]).astype(np.float32)
    both = jnp.concatenate([table, before % n_member], axis=0).astype(jnp.float32)
    wide = jnp.dot(both, spread).astype(i32)
    member = jnp.arange(n, dtype=i32) % n_member
    skip = (member[None, :] - wide[n:] + n_member) % n_member
    count = jnp.maximum((wide[:n] - skip + n_member - 1) // n_member, 0)
    turn_of = np.concatenate(
        [lane[:, None] == (lane ^ k)[None, :] for k in range(4)], axis=0
    ).astype(np.float32)
    turned = jnp.dot(turn_of, count.astype(jnp.float32)).astype(i32)
    views = [turned[k * n : (k + 1) * n] for k in range(4)]
    skip_mine = jnp.sum(jnp.where((source == me)[:, None], skip, 0), axis=0)

    w1 = min(4, slots)
    variants = [((), slots, slots)]
    caps = ()
    if slots == 32 and n_owner == 8 and n_member == 4:
        caps = (96, 48, 24)
        found = []
        for w, narrow in LEVELS:
            for pair in itertools.combinations(range(n_owner), 2):
                size = [w if o in pair else narrow for o in range(n_owner)]
                half = n_owner // 2
                cost = max(sum(size[:half]), sum(size[half:]))
                found.append((cost, pair, w, narrow))
        variants = [f[1:] for f in sorted(found)] + variants
    room = sum(caps)
    sizes = np.array(
        [[w if o in pair else narrow for o in range(n_owner)] for pair, w, narrow in variants],
        np.int32,
    )
    number = jnp.arange(len(variants), dtype=i32)
    choice = jnp.int32(0)
    if caps:
        widths = sorted({w for level in LEVELS for w in level})
        left, moved = flows([v[None] for v in views], jnp.asarray(widths, i32)[:, None, None], w1)
        tall = jnp.concatenate([left] + [moved[k][0] for k in range(3)], axis=1)
        short = jnp.dot(
            tall.reshape(-1, n).astype(jnp.float32), spread.T
        ).reshape(len(widths), 4 * n, n_owner)
        chosen = (sizes[:-1, None, :] == np.array(widths)[None, :, None]).astype(np.float32)
        load = jnp.einsum("vwo,wxo->vx", chosen, short)
        limit = np.repeat(np.array((0,) + caps), n).astype(np.float32)
        fits = jnp.all(load <= limit[None, :] + 0.5, axis=1)
        choice = jnp.min(jnp.where(fits, number[:-1], len(variants) - 1))
    picked = number[:, None] == choice
    w = jnp.sum(jnp.where(picked, np.repeat(sizes, n_member, axis=1), 0), axis=0)
    widest = jnp.max(w)
    _, moved = flows(views, w[None], w1)
    w_mine = jnp.sum(jnp.where(source == me, w, 0))

    here = source == me
    home = source // n_member

    def row(a):
        return jnp.sum(jnp.where(here[:, None], a, 0), axis=0)

    def running(a):
        return jnp.sum(jnp.where(source[None, :] < source[:, None], a[None, :], 0), axis=1)

    j = jnp.arange(slots, dtype=i32)[None, :]
    own = jnp.minimum(row(views[0]), w)
    first_of = home * capacity + skip_mine
    want = jnp.where(j < own[:, None], first_of[:, None] + j * n_member, -2)
    joins = jnp.zeros((n, slots), i32)
    leaves = []
    edge = jnp.maximum(own, w1)
    begin = own
    base = 0
    for k, cap in enumerate(caps):
        coming, going = row(moved[k][k + 1]), row(moved[k][0])
        inside = (j >= edge[:, None]) & (j < (edge + coming)[:, None])
        joins = jnp.where(inside, (examples + base + running(coming) - edge)[:, None] + j, joins)
        edge = edge + coming
        lo = running(going)
        t = jnp.arange(cap, dtype=i32)[:, None]
        inside = (t >= lo[None, :]) & (t < (lo + going)[None, :])
        at = (first_of + (begin - lo) * n_member)[None, :] + t * n_member + 1
        leaves.append(jnp.sum(jnp.where(inside, at, 0), axis=1) - 1)
        begin = begin + going
        base += cap
    want = jnp.concatenate([want.reshape(-1)] + leaves)

    code = jnp.where(keys // BIN_WIDTH >= cut[0], dest, -1)
    e = jnp.arange(examples, dtype=i32)
    local_rank = jnp.sum(
        (code[:, None] == code[None, :]) & (e[None, :] < e[:, None]), axis=1, dtype=i32
    )
    spot = jnp.where(code >= 0, code * capacity + local_rank, -9)
    match = jnp.sum(jnp.where(want[:, None] == spot[None, :], e[None, :], 0), axis=1)
    index = match[: n * slots] + joins.reshape(-1)
    spill_index = match[n * slots :] if caps else jnp.zeros((8,), i32)

    def column(a):
        return jnp.sum(jnp.where(here[None, :], a, 0), axis=1)

    mine_at = [column(v) for v in views]
    owned = [jnp.minimum(v, w_mine) for v in mine_at]
    first = jnp.sum(jnp.where(owners[None, :] == me_dp, before, 0), axis=1)
    first = (first - me_group + n_member - 1) // n_member
    near = jnp.minimum(owned[0], w1)
    block = n * w1 + source * (widest - w1) - w1
    spans = [(first, near, source * w1), (first + near, owned[0] - near, block + near)]
    at = first + owned[0]
    for k in range(len(caps)):
        going = column(moved[k][0])
        mate = k + 1
        slot = jnp.maximum(owned[mate], w1)
        for earlier in range(k):
            slot = slot + column(moved[earlier][mate ^ (earlier + 1)])
        there = jnp.bitwise_xor(source, mate)
        spans.append((at, going, n * w1 + there * (widest - w1) - w1 + slot))
        at = at + going
    lo = jnp.concatenate([s[0] for s in spans])
    size = jnp.concatenate([s[1] for s in spans])
    base = jnp.concatenate([s[2] for s in spans])
    t = jnp.arange(capacity, dtype=i32)[:, None]
    inside = (t >= lo[None, :]) & (t < (lo + size)[None, :])
    pick = jnp.sum(jnp.where(inside, t + (base - lo)[None, :] + 1, 0), axis=1)
    pick = jnp.where(pick > 0, pick - 1, capacity)

    def exchange(number):
        wide, w, narrow = variants[number]
        return pl.pallas_call(
            functools.partial(
                rows_kernel, n, n_member, slots, wide, w, narrow, w1, caps, pieces
            ),
            out_shape=(
                jax.ShapeDtypeStruct((capacity, pieces, LANES), jnp.int32),
                jax.ShapeDtypeStruct((BINS // LANES, LANES), jnp.float32),
                jax.ShapeDtypeStruct((capacity // LANES, LANES), jnp.float32),
            ),
            in_specs=[smem, smem, smem, hbm, vmem, vmem],
            out_specs=(hbm, vmem, vmem),
            scratch_shapes=[
                pltpu.VMEM((examples, pieces, LANES), jnp.int32),
                pltpu.VMEM((n * w, pieces, LANES), jnp.int32),
                pltpu.VMEM((max(room, 8), pieces, LANES), jnp.int32),
                pltpu.VMEM((max(room, 8), pieces, LANES), jnp.int32),
                pltpu.VMEM((n * per, LANES), jnp.int32),
                pltpu.VMEM((2 * BINS // LANES, LANES), jnp.bfloat16),
                pltpu.VMEM((BINS // LANES, LANES), jnp.float32),
            ]
            + [pltpu.SemaphoreType.DMA] * 6,
            compiler_params=pltpu.CompilerParams(
                collective_id=1 + number, has_side_effects=True,
                vmem_limit_bytes=60 * 1024 * 1024,
            ),
        )

    calls = [exchange(number) for number in range(len(variants))]
    choice, index, spill_index, pick, keys_all, owner_all = lax.optimization_barrier(
        (choice, index, spill_index, pick, keys_all, owner_all)
    )
    got, hist, weights = lax.switch(
        choice, calls, index, spill_index, cut, tokens, keys_all, owner_all
    )

    packed_rows = pl.pallas_call(
        functools.partial(pack_kernel, pieces, LANES),
        out_shape=jax.ShapeDtypeStruct((capacity, width), jnp.int32),
        in_specs=[smem, hbm],
        out_specs=hbm,
        scratch_shapes=[
            pltpu.VMEM((capacity + 1, pieces, LANES), jnp.int32),
            pltpu.VMEM((capacity, pieces, LANES), jnp.int32),
            pltpu.SemaphoreType.DMA,
            pltpu.SemaphoreType.DMA((capacity // LANES, pieces)),
        ],
        compiler_params=pltpu.CompilerParams(vmem_limit_bytes=60 * 1024 * 1024),
    )(pick, got)
    return (hist.reshape(BINS).astype(jnp.int32), packed_rows, weights.reshape(capacity))


def solution(mesh):
    placed = (P(("dp", "group")), P(), P(("dp", "group"), None), P(("dp", "group"), None))
    return jax.shard_map(
        functools.partial(body, mesh.shape["dp"], mesh.shape["group"]),
        mesh=mesh,
        in_specs=placed,
        out_specs=(P(), P(("dp", "group"), None), P(("dp", "group"))),
        check_vma=False,
    )
```

```python
import functools
import itertools

import jax
import jax.numpy as jnp
import numpy as np
from jax import lax
from jax.experimental import pallas as pl
from jax.experimental.pallas import tpu as pltpu
from jax.sharding import PartitionSpec as P

BINS = 4096
BIN_WIDTH = 262144
LANES = 128
LEVELS = ((28, 18), (31, 20))
MESH = pl.DeviceIdType.MESH


def peer(me, i, n):
    off = i + n // 2
    off = off - lax.div(off, n) * (n - 1)
    return lax.rem(me + off, n)


def place(d, n_member):
    return (lax.div(d, n_member), lax.rem(d, n_member))


def greet(me, n, n_member):
    barrier = pltpu.get_barrier_semaphore()

    def signal(i, c):
        pl.semaphore_signal(
            barrier, inc=1, device_id=place(peer(me, i, n), n_member), device_id_type=MESH
        )
        return c

    lax.fori_loop(0, n - 1, signal, 0)


def met(n):
    pl.semaphore_wait(pltpu.get_barrier_semaphore(), n - 1)


def meta_kernel(n, n_member, mine, every, local_sem, send_sem, recv_sem):
    me = lax.axis_index("dp") * n_member + lax.axis_index("group")
    own = pltpu.make_async_copy(mine, every.at[me], local_sem)
    own.start()
    greet(me, n, n_member)
    met(n)

    def start(i, c):
        d = peer(me, i, n)
        pltpu.make_async_remote_copy(
            src_ref=mine,
            dst_ref=every.at[me],
            send_sem=send_sem,
            recv_sem=recv_sem,
            device_id=place(d, n_member),
            device_id_type=MESH,
        ).start()
        return c

    lax.fori_loop(0, n - 1, start, 0)
    own.wait()
    rest = every.at[pl.ds(0, n - 1)]
    for sem in (send_sem, recv_sem):
        pltpu.make_async_copy(rest, rest, sem).wait()


def rows_kernel(
    n, n_member, slots, wide, w, narrow, w1, caps, pieces,
    index, spill_index, cut, tokens, every,
    got, hist, weights,
    held, send, leaving, joined, spot, table, tail,
    load_sem, own_sem, send_sem, recv_sem, leave_sem, join_sem,
):
    me_dp, me_group = lax.axis_index("dp"), lax.axis_index("group")
    me = me_dp * n_member + me_group
    spill = narrow < slots
    examples = held.shape[0]
    for p in range(pieces):
        pltpu.make_async_copy(
            tokens.at[:, pl.ds(p * LANES, LANES)], held.at[:, p, :], load_sem
        ).start()
    greet(me, n, n_member)
    pltpu.make_async_copy(got.at[pl.ds(0, examples)], held, load_sem).wait()

    def is_wide(d):
        at = lax.div(d, n_member)
        found = at == wide[0]
        for o in wide[1:]:
            found = jnp.logical_or(found, at == o)
        return found

    def fill1(d):
        for j in range(w1):
            send[d * w + j] = held[index[j, d]]

    def fill2(d, first, last):
        def one(j, c):
            at = index[j, d]
            if spill:
                local = held[jnp.minimum(at, examples - 1)]
                moved = joined[jnp.maximum(at - examples, 0)]
                send[d * w + j] = jnp.where(at < examples, local, moved)
            else:
                send[d * w + j] = held[at]
            return c

        lax.fori_loop(first, last, one, 0)

    def remote(src, dst, out_sem, in_sem, d):
        return pltpu.make_async_remote_copy(
            src_ref=src, dst_ref=dst, send_sem=out_sem, recv_sem=in_sem,
            device_id=place(d, n_member), device_id_type=MESH,
        )

    def part1(d, at):
        return remote(
            send.at[pl.ds(d * w, w1)], got.at[pl.ds(at * w1, w1)], send_sem, recv_sem, d
        )

    def part2(d, at):
        return remote(
            send.at[pl.ds(d * w + w1, narrow - w1)],
            got.at[pl.ds(n * w1 + at * (w - w1), narrow - w1)], send_sem, recv_sem, d,
        )

    def part3(d, at):
        return remote(
            send.at[pl.ds(d * w + narrow, w - narrow)],
            got.at[pl.ds(n * w1 + at * (w - w1) + narrow - w1, w - narrow)],
            send_sem, recv_sem, d,
        )

    def when_wide(d, act):
        if wide:
            pl.when(is_wide(d))(act)

    moves = []
    if spill:
        base = me_group - lax.rem(me_group, 4)
        mine = me_group - base
        core, column = lax.rem(mine, 2), lax.div(mine, 2)
        begin = 0
        for k, cap in enumerate(caps):
            other = base + (column if k == 0 else 1 - column) * 2 + (core if k == 1 else 1 - core)
            rows = pl.ds(begin, cap)
            moves.append(
                remote(
                    leaving.at[rows], joined.at[rows], leave_sem, join_sem,
                    me_dp * n_member + other,
                )
            )
            begin += cap

        def leave(g, c):
            for j in range(4):
                at = g * 4 + j
                leaving[at] = held[spill_index[0, at]]
            return c

        lax.fori_loop(0, begin // 4, leave, 0)
    met(n)
    for move in moves:
        move.start()

    def start1(i, c):
        d = peer(me, i, n)
        fill1(d)
        part1(d, me).start()
        return c

    lax.fori_loop(0, n - 1, start1, 0)
    if spill:
        everything = pl.ds(0, sum(caps))
        pltpu.make_async_copy(leaving.at[everything], joined.at[everything], join_sem).wait()

    def start2(i, c):
        d = peer(me, i, n)
        fill2(d, w1, narrow)
        part2(d, me).start()

        def rest():
            fill2(d, narrow, w)
            part3(d, me).start()

        when_wide(d, rest)
        return c

    lax.fori_loop(0, n - 1, start2, 0)
    fill1(me)
    fill2(me, w1, w)
    owns = [
        pltpu.make_async_copy(
            send.at[pl.ds(me * w, w1)], got.at[pl.ds(me * w1, w1)], own_sem
        ),
        pltpu.make_async_copy(
            send.at[pl.ds(me * w + w1, w - w1)],
            got.at[pl.ds(n * w1 + me * (w - w1), w - w1)], own_sem,
        ),
    ]
    for own in owns:
        own.start()

    per = every.shape[1] // 2

    def line(r, first):
        return every[lax.div(r, per), pl.ds(lax.rem(r, per) + first, 1), :]

    hist[...] = jnp.zeros_like(hist)
    tail[...] = jnp.zeros_like(tail)
    hi_of = lax.broadcasted_iota(jnp.int32, (BINS // LANES, LANES), 0)
    lo_of = lax.broadcasted_iota(jnp.int32, (LANES, LANES), 0)
    row_of = lax.broadcasted_iota(jnp.int32, (LANES, LANES), 0)
    lane_of = lax.broadcasted_iota(jnp.int32, (LANES, LANES), 1)
    earlier = jnp.where(row_of < lane_of, 1.0, 0.0).astype(jnp.bfloat16)
    ones = jnp.ones((LANES, LANES), jnp.bfloat16)

    def count(r, seen):
        bins = line(r, 0) // BIN_WIDTH
        hi = jnp.where(hi_of == bins // LANES, 1.0, 0.0).astype(jnp.bfloat16)
        lo = jnp.where(lo_of == bins % LANES, 1.0, 0.0).astype(jnp.bfloat16)
        hist[...] += lax.dot_general(
            hi, lo, (((1,), (1,)), ((), ())), preferred_element_type=jnp.float32
        )
        above = jnp.where(hi_of < bins // LANES, 1.0, 0.0).astype(jnp.bfloat16)
        reach = jnp.where(lo_of <= bins % LANES, 1.0, 0.0).astype(jnp.bfloat16)
        tail[...] += lax.dot_general(
            hi, reach, (((1,), (1,)), ((), ())), preferred_element_type=jnp.float32
        ) + lax.dot_general(
            above, ones, (((1,), (0,)), ((), ())), preferred_element_type=jnp.float32
        )
        mine = jnp.logical_and(line(r, per) == me_dp, bins >= cut[0])
        flags = jnp.where(mine, 1.0, 0.0)
        eight = jnp.broadcast_to(flags, (8, LANES)).astype(jnp.bfloat16)
        below = lax.dot_general(
            eight, earlier, (((1,), (0,)), ((), ())), preferred_element_type=jnp.float32
        )[0:1]
        whole = lax.dot_general(
            eight, ones, (((1,), (0,)), ((), ())), preferred_element_type=jnp.float32
        )[0:1]
        rank = (below + seen).astype(jnp.int32)
        here = jnp.logical_and(mine, rank % n_member == me_group)
        spot[pl.ds(r, 1), :] = jnp.where(here, rank // n_member, -1)
        return seen + whole

    lax.fori_loop(0, n * per, count, jnp.zeros((1, LANES), jnp.float32))

    suffix = tail[...]
    upper = jnp.floor(suffix * (1.0 / LANES))
    table[...] = jnp.concatenate([upper, suffix - upper * LANES], axis=0).astype(jnp.bfloat16)
    bin_of = hi_of * LANES + lax.broadcasted_iota(jnp.int32, hi_of.shape, 1)
    kept = jnp.sum(
        jnp.sum(jnp.where(bin_of == cut[0], suffix, 0.0), axis=1, keepdims=True),
        axis=0, keepdims=True,
    )
    total = jnp.maximum(kept, 1.0)
    groups = weights.shape[0]
    group_of = lax.broadcasted_iota(jnp.int32, (groups, LANES), 0)
    weights[...] = jnp.zeros_like(weights)

    def weigh(r, c):
        bins = line(r, 0) // BIN_WIDTH
        slot = spot[pl.ds(r, 1), :]
        lo = jnp.where(lo_of == bins % LANES, 1.0, 0.0).astype(jnp.bfloat16)
        rows = lax.dot_general(
            table[...], lo, (((1,), (0,)), ((), ())), preferred_element_type=jnp.float32
        )
        pick = hi_of == bins // LANES
        up = jnp.sum(jnp.where(pick, rows[: BINS // LANES], 0.0), axis=0, keepdims=True)
        down = jnp.sum(jnp.where(pick, rows[BINS // LANES :], 0.0), axis=0, keepdims=True)
        at = jnp.logical_and(slot >= 0, group_of == slot // LANES)
        column = jnp.where(lo_of == slot % LANES, 1.0, 0.0).astype(jnp.bfloat16)
        both = jnp.concatenate([jnp.where(at, up, 0.0), jnp.where(at, down, 0.0)], axis=0)
        laid = lax.dot_general(
            both.astype(jnp.bfloat16), column, (((1,), (1,)), ((), ())),
            preferred_element_type=jnp.float32,
        )
        weights[...] += laid[:groups] * LANES + laid[groups:]
        return c

    lax.fori_loop(0, n * per, weigh, 0)
    weights[...] = weights[...] / total

    def done(rows, sem):
        rows = pl.ds(0, rows)
        pltpu.make_async_copy(send.at[rows], got.at[rows], sem).wait()

    done(w, own_sem)
    if spill:
        pltpu.make_async_copy(leaving.at[everything], joined.at[everything], leave_sem).wait()
    out = (n - len(wide) * n_member) * narrow + len(wide) * n_member * w
    if wide:
        def ends(size):
            done(out - size, send_sem)
            done((n - 1) * size, recv_sem)

        pl.when(is_wide(me))(functools.partial(ends, w))
        pl.when(jnp.logical_not(is_wide(me)))(functools.partial(ends, narrow))
    else:
        done(out - w, send_sem)
        done((n - 1) * w, recv_sem)


def pack_kernel(pieces, chunk, index, got, out, held, made, load_sem, out_sem):
    rows = got.shape[0]
    slots = made.shape[0]
    load = pltpu.make_async_copy(got, held.at[pl.ds(0, rows)], load_sem)
    load.start()
    held[rows] = jnp.zeros(held.shape[1:], jnp.int32)
    load.wait()

    def stores(k):
        return [
            pltpu.make_async_copy(
                made.at[pl.ds(k * chunk, chunk), p, :],
                out.at[pl.ds(k * chunk, chunk), pl.ds(p * LANES, LANES)],
                out_sem.at[k, p],
            )
            for p in range(pieces)
        ]

    def fill(k):
        def some(g, c):
            for j in range(8):
                s = k * chunk + g * 8 + j
                made[s] = held[index[0, s]]
            return c

        lax.fori_loop(0, chunk // 8, some, 0)

    def step(k, c):
        fill(k)
        for copy in stores(k):
            copy.start()
        return c

    def finish(k, c):
        for copy in stores(k):
            copy.wait()
        return c

    lax.fori_loop(0, slots // chunk, step, 0)
    lax.fori_loop(0, slots // chunk, finish, 0)


def flows(views, w, w1):
    over = [jnp.maximum(v - w, 0) for v in views]
    free = [w - jnp.maximum(jnp.minimum(v, w), w1) for v in views]
    moved = []
    for step in (1, 2, 3):
        flow = [jnp.minimum(over[k], free[k ^ step]) for k in range(4)]
        over = [over[k] - flow[k] for k in range(4)]
        free = [free[k] - flow[k ^ step] for k in range(4)]
        moved.append(flow)
    return over[0], moved


def plan_kernel(
    n, n_member, slots, w1, caps, levels, cut, every, pairs, order,
    choice, index, spill_index, pick, rows_of,
):
    f32, i32, bf16 = jnp.float32, jnp.int32, jnp.bfloat16
    per = every.shape[1] // 2
    examples = per * LANES
    capacity = 2 * examples
    n_owner = n // n_member
    me_dp, me_group = lax.axis_index("dp"), lax.axis_index("group")
    me = me_dp * n_member + me_group

    def iota(shape, axis):
        return lax.broadcasted_iota(i32, shape, axis)

    def mm(a, b, dims=(((1,), (0,)), ((), ()))):
        return lax.dot_general(
            a.astype(bf16), b.astype(bf16), dims, preferred_element_type=f32
        )

    def one(flag):
        return jnp.where(flag, 1.0, 0.0)

    def rows(a):
        return jnp.sum(a, axis=0, keepdims=True)

    def lanes(a):
        return jnp.sum(a, axis=1, keepdims=True)

    side = ((((1,), (1,)), ((), ())))
    lane = iota((n, LANES), 1)
    home = lane // n_member
    member = lane % n_member
    src = iota((n, LANES), 0)
    small_r, small_c = iota((n, n), 0), iota((n, n), 1)

    kept = every[:, :per, :] // BIN_WIDTH >= cut[0]
    code = jnp.where(kept, every[:, per:, :], -1)
    table = jnp.zeros((n, LANES), f32)
    for o in range(n_owner):
        total = lanes(jnp.sum(one(code == o), axis=1))
        table = jnp.where(home == o, total, table)
    before = mm(one(small_c < small_r), table).astype(i32)
    skip = (member - before) & (n_member - 1)
    count = (table.astype(i32) - skip + n_member - 1) // n_member
    views = [count] + [
        mm(one(small_c == (small_r ^ k)), count.astype(f32)).astype(i32) for k in (1, 2, 3)
    ]

    sets = {}
    for width in sorted({w for level in levels for w in level}):
        left, moved = flows(views, width, w1)
        sets[width] = jnp.concatenate([left] + [moved[k][0] for k in range(3)], axis=0).astype(f32)
    col = iota((32, 4 * n), 1) // n
    limit = jnp.where(col == 0, 0.5, 0.0)
    for k, cap in enumerate(caps):
        limit = jnp.where(col == k + 1, cap + 0.5, limit)
    member_of = pairs[...]
    last = len(levels) * 28
    best = jnp.full((1, 1), last, i32)
    for number, (wide, narrow) in enumerate(levels):
        load = mm(member_of, sets[wide], side) + mm(1.0 - member_of, sets[narrow], side)
        bad = lanes(one(load > limit))
        rank = jnp.where(bad > 0.5, last, order[number][:, :1])
        best = jnp.minimum(best, jnp.min(rank, axis=0, keepdims=True))
    choice[...] = jnp.broadcast_to(best, choice.shape)
    w = jnp.zeros((1, LANES), f32)
    widest = jnp.zeros((1, 1), f32)
    for number, (wide, narrow) in enumerate(levels):
        hit = one(order[number] == best)
        found = rows(hit[:, :1])
        w = w + rows(hit * member_of) * (wide - narrow) + found * narrow
        widest = widest + found * wide
    w = jnp.where(best == last, float(slots), w).astype(i32)
    widest = jnp.where(best == last, float(slots), widest).astype(i32)
    _, moved = flows(views, w, w1)

    def row(a):
        return rows(jnp.where(src == me, a, 0))

    square_r, square_c = iota((LANES, LANES), 0), iota((LANES, LANES), 1)
    earlier = one(square_r < square_c)

    def running(a):
        return mm(jnp.broadcast_to(a.astype(f32), (8, LANES)), earlier)[:1].astype(i32)

    mine = every[me]
    my_code = jnp.where(mine[:per] // BIN_WIDTH >= cut[0], mine[per:], -1)
    owner_of = iota((n_owner, LANES), 0)
    seen = jnp.zeros((n_owner, 1), f32)
    found = jnp.zeros((LANES, LANES), i32)
    for r in range(per):
        line = my_code[r : r + 1]
        hot = one(owner_of == line)
        rank = rows(hot * (mm(hot, earlier) + seen)).astype(i32)
        rank = jnp.where(line >= 0, rank, -1)
        seen = seen + lanes(hot)
        at = one(square_r == rank)
        to = jnp.where(square_r // n_member == line, (square_c + 1).astype(f32), 0.0)
        got = mm(at, to, side).astype(i32)
        found = found + jnp.where(got > 0, got + r * LANES, 0)
    rows_of[...] = found

    own = jnp.minimum(row(views[0]), w)
    my_skip = row(skip)
    j = iota((slots, LANES), 0)
    local = jnp.zeros((slots, LANES), i32)
    for r in range(n_member):
        local = jnp.where(my_skip == r, rows_of[pl.ds(r, slots, stride=n_member), :], local)
    slot_row = jnp.where(j < own, jnp.maximum(local - 1, 0), 0)
    edge = jnp.maximum(own, w1)
    begin = own
    base = 0
    down = []
    inner = []
    for k, cap in enumerate(caps):
        coming, going = row(moved[k][k + 1]), row(moved[k][0])
        inside = (j >= edge) & (j < edge + coming)
        slot_row = jnp.where(inside, examples + base + running(coming) - edge + j, slot_row)
        edge = edge + coming
        lo = running(going)
        t = iota((cap, LANES), 0)
        inside = (t >= lo) & (t < lo + going)
        inner.append(one(inside))
        down.append(lanes(jnp.where(inside, my_skip + (begin - lo + t) * n_member + 1, 0)) - 1)
        begin = begin + going
        base += cap
    index[...] = slot_row
    inner = jnp.concatenate(inner, axis=0)
    down = jnp.concatenate(down, axis=0)
    room = sum(caps)
    hot = one(iota((room, LANES), 1) == down)
    high = found // LANES
    spread = mm(hot, high.astype(f32)) * LANES + mm(hot, (found - high * LANES).astype(f32))
    value = jnp.maximum(lanes(spread * inner) - 1.0, 0.0)
    turned = rows(jnp.where(iota((room, 256), 0) == iota((room, 256), 1), value, 0.0))
    spill_index[...] = turned.astype(i32)

    def column(a):
        return lanes(jnp.where(lane == me, a, 0))

    w_mine = lanes(jnp.where(lane[:1] == me, w, 0))
    owned = [jnp.minimum(column(v), w_mine) for v in views]
    source = iota((n, 1), 0)
    first = (column(before) - me_group + n_member - 1) // n_member
    near = jnp.minimum(owned[0], w1)
    block = n * w1 + source * (widest - w1) - w1
    spans = [(first, near, source * w1), (first + near, owned[0] - near, block + near)]
    at = first + owned[0]
    for k in range(len(caps)):
        going = column(moved[k][0])
        mate = k + 1
        slot = jnp.maximum(owned[mate], w1)
        for before_k in range(k):
            slot = slot + column(moved[before_k][mate ^ (before_k + 1)])
        spans.append((at, going, n * w1 + (source ^ mate) * (widest - w1) - w1 + slot))
        at = at + going
    t = iota((n, capacity), 1)
    where = jnp.zeros((n, capacity), i32)
    for lo, size, to in spans:
        where = where + jnp.where((t >= lo) & (t < lo + size), t + (to - lo + 1), 0)
    where = rows(where)
    pick[...] = jnp.where(where > 0, where - 1, capacity)


def body(n_owner, n_member, keys, cut, owner, tokens):
    examples, width = tokens.shape
    n = n_owner * n_member
    slots = 2 * examples // n
    capacity = 2 * examples
    pieces = width // LANES
    per = examples // LANES
    me_dp, me_group = lax.axis_index("dp"), lax.axis_index("group")
    me = me_dp * n_member + me_group
    vmem = pl.BlockSpec(memory_space=pltpu.VMEM)
    smem = pl.BlockSpec(memory_space=pltpu.SMEM)
    hbm = pl.BlockSpec(memory_space=pl.ANY)
    dest = owner[:, 0]
    i32 = jnp.int32

    mine = jnp.concatenate([keys.reshape(per, LANES), dest.reshape(per, LANES)], axis=0)
    every = pl.pallas_call(
        functools.partial(meta_kernel, n, n_member),
        out_shape=jax.ShapeDtypeStruct((n, 2 * per, LANES), jnp.int32),
        in_specs=[vmem],
        out_specs=vmem,
        scratch_shapes=[
            pltpu.SemaphoreType.DMA,
            pltpu.SemaphoreType.DMA,
            pltpu.SemaphoreType.DMA,
        ],
        compiler_params=pltpu.CompilerParams(collective_id=0, has_side_effects=True),
    )(mine)
    w1 = min(4, slots)
    variants = [((), slots, slots)]
    caps = ()
    if slots == 32 and n_owner == 8 and n_member == 4:
        caps = (96, 48, 24)
        found = []
        for w, narrow in LEVELS:
            for pair in itertools.combinations(range(n_owner), 2):
                size = [w if o in pair else narrow for o in range(n_owner)]
                half = n_owner // 2
                cost = max(sum(size[:half]), sum(size[half:]))
                found.append((cost, pair, w, narrow))
        variants = [f[1:] for f in sorted(found)] + variants
    room = sum(caps)
    sizes = np.array(
        [[w if o in pair else narrow for o in range(n_owner)] for pair, w, narrow in variants],
        np.int32,
    )
    if caps:
        order = np.full((len(LEVELS), 32, LANES), len(variants), np.int32)
        pairs = np.zeros((32, LANES), np.float32)
        for p, pair in enumerate(itertools.combinations(range(n_owner), 2)):
            for o in pair:
                pairs[p, o * n_member : (o + 1) * n_member] = 1
            for at, level in enumerate(LEVELS):
                order[at, p] = variants.index((pair,) + level)
        choice, index, spill_index, pick = pl.pallas_call(
            functools.partial(plan_kernel, n, n_member, slots, w1, caps, LEVELS),
            out_shape=(
                jax.ShapeDtypeStruct((8, LANES), i32),
                jax.ShapeDtypeStruct((slots, LANES), i32),
                jax.ShapeDtypeStruct((1, 256), i32),
                jax.ShapeDtypeStruct((1, capacity), i32),
            ),
            in_specs=[smem, vmem, vmem, vmem],
            out_specs=(vmem,) * 4,
            scratch_shapes=[pltpu.VMEM((LANES, LANES), i32)],
        )(cut, every, jnp.asarray(pairs), jnp.asarray(order))
        choice = choice[0, 0]
    else:
        keys_all = every[:, :per].reshape(n * per, LANES)
        owner_all = every[:, per:].reshape(n * per, LANES)
        code_all = jnp.where(keys_all // BIN_WIDTH >= cut[0], owner_all, -1).reshape(n, examples)
        owners = jnp.arange(n_owner, dtype=i32)
        table = jnp.sum(code_all[:, None, :] == owners[None, :, None], axis=2, dtype=i32)
        source = jnp.arange(n, dtype=i32)
        before = jnp.sum(
            jnp.where((source[None, :] < source[:, None])[:, :, None], table[None], 0), axis=1
        )

        lane = np.arange(n)
        spread = (lane[None, :] // n_member == np.arange(n_owner)[:, None]).astype(np.float32)
        both = jnp.concatenate([table, before % n_member], axis=0).astype(jnp.float32)
        wide = jnp.dot(both, spread).astype(i32)
        member = jnp.arange(n, dtype=i32) % n_member
        skip = (member[None, :] - wide[n:] + n_member) % n_member
        count = jnp.maximum((wide[:n] - skip + n_member - 1) // n_member, 0)
        turn_of = np.concatenate(
            [lane[:, None] == (lane ^ k)[None, :] for k in range(4)], axis=0
        ).astype(np.float32)
        turned = jnp.dot(turn_of, count.astype(jnp.float32)).astype(i32)
        views = [turned[k * n : (k + 1) * n] for k in range(4)]
        skip_mine = jnp.sum(jnp.where((source == me)[:, None], skip, 0), axis=0)

        number = jnp.arange(len(variants), dtype=i32)
        choice = jnp.int32(0)
        picked = number[:, None] == choice
        w = jnp.sum(jnp.where(picked, np.repeat(sizes, n_member, axis=1), 0), axis=0)
        widest = jnp.max(w)
        _, moved = flows(views, w[None], w1)
        w_mine = jnp.sum(jnp.where(source == me, w, 0))

        here = source == me
        home = source // n_member

        def row(a):
            return jnp.sum(jnp.where(here[:, None], a, 0), axis=0)

        def running(a):
            return jnp.sum(jnp.where(source[None, :] < source[:, None], a[None, :], 0), axis=1)

        j = jnp.arange(slots, dtype=i32)[None, :]
        own = jnp.minimum(row(views[0]), w)
        first_of = home * capacity + skip_mine
        want = jnp.where(j < own[:, None], first_of[:, None] + j * n_member, -2)
        joins = jnp.zeros((n, slots), i32)
        leaves = []
        edge = jnp.maximum(own, w1)
        begin = own
        base = 0
        for k, cap in enumerate(caps):
            coming, going = row(moved[k][k + 1]), row(moved[k][0])
            inside = (j >= edge[:, None]) & (j < (edge + coming)[:, None])
            joins = jnp.where(inside, (examples + base + running(coming) - edge)[:, None] + j, joins)
            edge = edge + coming
            lo = running(going)
            t = jnp.arange(cap, dtype=i32)[:, None]
            inside = (t >= lo[None, :]) & (t < (lo + going)[None, :])
            at = (first_of + (begin - lo) * n_member)[None, :] + t * n_member + 1
            leaves.append(jnp.sum(jnp.where(inside, at, 0), axis=1) - 1)
            begin = begin + going
            base += cap
        want = jnp.concatenate([want.reshape(-1)] + leaves)

        code = jnp.where(keys // BIN_WIDTH >= cut[0], dest, -1)
        e = jnp.arange(examples, dtype=i32)
        local_rank = jnp.sum(
            (code[:, None] == code[None, :]) & (e[None, :] < e[:, None]), axis=1, dtype=i32
        )
        spot = jnp.where(code >= 0, code * capacity + local_rank, -9)
        match = jnp.sum(jnp.where(want[:, None] == spot[None, :], e[None, :], 0), axis=1)
        index = match[: n * slots] + joins.reshape(-1)
        spill_index = match[n * slots :] if caps else jnp.zeros((8,), i32)

        def column(a):
            return jnp.sum(jnp.where(here[None, :], a, 0), axis=1)

        mine_at = [column(v) for v in views]
        owned = [jnp.minimum(v, w_mine) for v in mine_at]
        first = jnp.sum(jnp.where(owners[None, :] == me_dp, before, 0), axis=1)
        first = (first - me_group + n_member - 1) // n_member
        near = jnp.minimum(owned[0], w1)
        block = n * w1 + source * (widest - w1) - w1
        spans = [(first, near, source * w1), (first + near, owned[0] - near, block + near)]
        at = first + owned[0]
        for k in range(len(caps)):
            going = column(moved[k][0])
            mate = k + 1
            slot = jnp.maximum(owned[mate], w1)
            for earlier in range(k):
                slot = slot + column(moved[earlier][mate ^ (earlier + 1)])
            there = jnp.bitwise_xor(source, mate)
            spans.append((at, going, n * w1 + there * (widest - w1) - w1 + slot))
            at = at + going
        lo = jnp.concatenate([s[0] for s in spans])
        size = jnp.concatenate([s[1] for s in spans])
        base = jnp.concatenate([s[2] for s in spans])
        t = jnp.arange(capacity, dtype=i32)[:, None]
        inside = (t >= lo[None, :]) & (t < (lo + size)[None, :])
        pick = jnp.sum(jnp.where(inside, t + (base - lo)[None, :] + 1, 0), axis=1)
        pick = jnp.where(pick > 0, pick - 1, capacity)
        index = index.reshape(n, slots).T
        spill_index, pick = spill_index[None], pick[None]

    def exchange(number):
        wide, w, narrow = variants[number]
        return pl.pallas_call(
            functools.partial(
                rows_kernel, n, n_member, slots, wide, w, narrow, w1, caps, pieces
            ),
            out_shape=(
                jax.ShapeDtypeStruct((capacity, pieces, LANES), jnp.int32),
                jax.ShapeDtypeStruct((BINS // LANES, LANES), jnp.float32),
                jax.ShapeDtypeStruct((capacity // LANES, LANES), jnp.float32),
            ),
            in_specs=[smem, smem, smem, hbm, vmem],
            out_specs=(hbm, vmem, vmem),
            scratch_shapes=[
                pltpu.VMEM((examples, pieces, LANES), jnp.int32),
                pltpu.VMEM((n * w, pieces, LANES), jnp.int32),
                pltpu.VMEM((max(room, 8), pieces, LANES), jnp.int32),
                pltpu.VMEM((max(room, 8), pieces, LANES), jnp.int32),
                pltpu.VMEM((n * per, LANES), jnp.int32),
                pltpu.VMEM((2 * BINS // LANES, LANES), jnp.bfloat16),
                pltpu.VMEM((BINS // LANES, LANES), jnp.float32),
            ]
            + [pltpu.SemaphoreType.DMA] * 6,
            compiler_params=pltpu.CompilerParams(
                collective_id=1 + number, has_side_effects=True,
                vmem_limit_bytes=60 * 1024 * 1024,
            ),
        )

    calls = [exchange(number) for number in range(len(variants))]
    choice, index, spill_index, pick = lax.optimization_barrier(
        (choice, index, spill_index, pick)
    )
    got, hist, weights = lax.switch(
        choice, calls, index, spill_index, cut, tokens, every
    )

    packed_rows = pl.pallas_call(
        functools.partial(pack_kernel, pieces, LANES),
        out_shape=jax.ShapeDtypeStruct((capacity, width), jnp.int32),
        in_specs=[smem, hbm],
        out_specs=hbm,
        scratch_shapes=[
            pltpu.VMEM((capacity + 1, pieces, LANES), jnp.int32),
            pltpu.VMEM((capacity, pieces, LANES), jnp.int32),
            pltpu.SemaphoreType.DMA,
            pltpu.SemaphoreType.DMA((capacity // LANES, pieces)),
        ],
        compiler_params=pltpu.CompilerParams(vmem_limit_bytes=60 * 1024 * 1024),
    )(pick, got)
    return (hist.reshape(BINS).astype(jnp.int32), packed_rows, weights.reshape(capacity))


def solution(mesh):
    placed = (P(("dp", "group")), P(), P(("dp", "group"), None), P(("dp", "group"), None))
    return jax.shard_map(
        functools.partial(body, mesh.shape["dp"], mesh.shape["group"]),
        mesh=mesh,
        in_specs=placed,
        out_specs=(P(), P(("dp", "group"), None), P(("dp", "group"))),
        check_vma=False,
    )
```

```python
import functools
import itertools

import jax
import jax.numpy as jnp
import numpy as np
from jax import lax
from jax.experimental import pallas as pl
from jax.experimental.pallas import tpu as pltpu
from jax.sharding import PartitionSpec as P

BINS = 4096
BIN_WIDTH = 262144
LANES = 128
LEVELS = ((28, 18), (31, 20))
MESH = pl.DeviceIdType.MESH


def peer(me, i, n):
    off = i + n // 2
    off = off - lax.div(off, n) * (n - 1)
    return lax.rem(me + off, n)


def place(d, n_member):
    return (lax.div(d, n_member), lax.rem(d, n_member))


def greet(me, n, n_member):
    barrier = pltpu.get_barrier_semaphore()

    def signal(i, c):
        pl.semaphore_signal(
            barrier, inc=1, device_id=place(peer(me, i, n), n_member), device_id_type=MESH
        )
        return c

    lax.fori_loop(0, n - 1, signal, 0)


def met(n):
    pl.semaphore_wait(pltpu.get_barrier_semaphore(), n - 1)


def meta_kernel(n, n_member, mine, every, local_sem, send_sem, recv_sem):
    me = lax.axis_index("dp") * n_member + lax.axis_index("group")
    own = pltpu.make_async_copy(mine, every.at[me], local_sem)
    own.start()
    greet(me, n, n_member)
    met(n)

    def start(i, c):
        d = peer(me, i, n)
        pltpu.make_async_remote_copy(
            src_ref=mine,
            dst_ref=every.at[me],
            send_sem=send_sem,
            recv_sem=recv_sem,
            device_id=place(d, n_member),
            device_id_type=MESH,
        ).start()
        return c

    lax.fori_loop(0, n - 1, start, 0)
    own.wait()
    rest = every.at[pl.ds(0, n - 1)]
    for sem in (send_sem, recv_sem):
        pltpu.make_async_copy(rest, rest, sem).wait()


def rows_kernel(
    n, n_member, slots, wide, w, narrow, w1, caps, pieces,
    index, spill_index, cut, tokens, every,
    got, hist, weights,
    held, send, leaving, joined, spot, table, tail,
    load_sem, own_sem, send_sem, recv_sem, leave_sem, join_sem,
):
    me_dp, me_group = lax.axis_index("dp"), lax.axis_index("group")
    me = me_dp * n_member + me_group
    spill = narrow < slots
    examples = held.shape[0]
    for p in range(pieces):
        pltpu.make_async_copy(
            tokens.at[:, pl.ds(p * LANES, LANES)], held.at[:, p, :], load_sem
        ).start()
    greet(me, n, n_member)
    pltpu.make_async_copy(got.at[pl.ds(0, examples)], held, load_sem).wait()

    def is_wide(d):
        at = lax.div(d, n_member)
        found = at == wide[0]
        for o in wide[1:]:
            found = jnp.logical_or(found, at == o)
        return found

    def fill1(d):
        for j in range(w1):
            send[d * w + j] = held[index[j, d]]

    def fill2(d, first, last):
        def one(j, c):
            at = index[j, d]
            if spill:
                local = held[jnp.minimum(at, examples - 1)]
                moved = joined[jnp.maximum(at - examples, 0)]
                send[d * w + j] = jnp.where(at < examples, local, moved)
            else:
                send[d * w + j] = held[at]
            return c

        lax.fori_loop(first, last, one, 0)

    def remote(src, dst, out_sem, in_sem, d):
        return pltpu.make_async_remote_copy(
            src_ref=src, dst_ref=dst, send_sem=out_sem, recv_sem=in_sem,
            device_id=place(d, n_member), device_id_type=MESH,
        )

    def part1(d, at):
        return remote(
            send.at[pl.ds(d * w, w1)], got.at[pl.ds(at * w1, w1)], send_sem, recv_sem, d
        )

    def part2(d, at):
        return remote(
            send.at[pl.ds(d * w + w1, narrow - w1)],
            got.at[pl.ds(n * w1 + at * (w - w1), narrow - w1)], send_sem, recv_sem, d,
        )

    def part3(d, at):
        return remote(
            send.at[pl.ds(d * w + narrow, w - narrow)],
            got.at[pl.ds(n * w1 + at * (w - w1) + narrow - w1, w - narrow)],
            send_sem, recv_sem, d,
        )

    def when_wide(d, act):
        if wide:
            pl.when(is_wide(d))(act)

    moves = []
    if spill:
        base = me_group - lax.rem(me_group, 4)
        mine = me_group - base
        core, column = lax.rem(mine, 2), lax.div(mine, 2)
        begin = 0
        for k, cap in enumerate(caps):
            other = base + (column if k == 0 else 1 - column) * 2 + (core if k == 1 else 1 - core)
            rows = pl.ds(begin, cap)
            moves.append(
                remote(
                    leaving.at[rows], joined.at[rows], leave_sem, join_sem,
                    me_dp * n_member + other,
                )
            )
            begin += cap

        def leave(g, c):
            for j in range(4):
                at = g * 4 + j
                leaving[at] = held[spill_index[0, at]]
            return c

        lax.fori_loop(0, begin // 4, leave, 0)
    met(n)
    for move in moves:
        move.start()

    def start1(i, c):
        d = peer(me, i, n)
        fill1(d)
        part1(d, me).start()
        return c

    lax.fori_loop(0, n - 1, start1, 0)
    if spill:
        everything = pl.ds(0, sum(caps))
        pltpu.make_async_copy(leaving.at[everything], joined.at[everything], join_sem).wait()

    def start2(i, c):
        d = peer(me, i, n)
        fill2(d, w1, narrow)
        part2(d, me).start()

        def rest():
            fill2(d, narrow, w)
            part3(d, me).start()

        when_wide(d, rest)
        return c

    lax.fori_loop(0, n - 1, start2, 0)
    fill1(me)
    fill2(me, w1, w)
    owns = [
        pltpu.make_async_copy(
            send.at[pl.ds(me * w, w1)], got.at[pl.ds(me * w1, w1)], own_sem
        ),
        pltpu.make_async_copy(
            send.at[pl.ds(me * w + w1, w - w1)],
            got.at[pl.ds(n * w1 + me * (w - w1), w - w1)], own_sem,
        ),
    ]
    for own in owns:
        own.start()

    per = every.shape[1] // 2

    def line(r, first):
        return every[lax.div(r, per), pl.ds(lax.rem(r, per) + first, 1), :]

    hist[...] = jnp.zeros_like(hist)
    tail[...] = jnp.zeros_like(tail)
    hi_of = lax.broadcasted_iota(jnp.int32, (BINS // LANES, LANES), 0)
    lo_of = lax.broadcasted_iota(jnp.int32, (LANES, LANES), 0)
    row_of = lax.broadcasted_iota(jnp.int32, (LANES, LANES), 0)
    lane_of = lax.broadcasted_iota(jnp.int32, (LANES, LANES), 1)
    earlier = jnp.where(row_of < lane_of, 1.0, 0.0).astype(jnp.bfloat16)
    ones = jnp.ones((LANES, LANES), jnp.bfloat16)

    def count(r, seen):
        bins = line(r, 0) // BIN_WIDTH
        hi = jnp.where(hi_of == bins // LANES, 1.0, 0.0).astype(jnp.bfloat16)
        lo = jnp.where(lo_of == bins % LANES, 1.0, 0.0).astype(jnp.bfloat16)
        hist[...] += lax.dot_general(
            hi, lo, (((1,), (1,)), ((), ())), preferred_element_type=jnp.float32
        ).astype(jnp.int32)
        above = jnp.where(hi_of < bins // LANES, 1.0, 0.0).astype(jnp.bfloat16)
        reach = jnp.where(lo_of <= bins % LANES, 1.0, 0.0).astype(jnp.bfloat16)
        tail[...] += lax.dot_general(
            hi, reach, (((1,), (1,)), ((), ())), preferred_element_type=jnp.float32
        ) + lax.dot_general(
            above, ones, (((1,), (0,)), ((), ())), preferred_element_type=jnp.float32
        )
        mine = jnp.logical_and(line(r, per) == me_dp, bins >= cut[0])
        flags = jnp.where(mine, 1.0, 0.0)
        eight = jnp.broadcast_to(flags, (8, LANES)).astype(jnp.bfloat16)
        below = lax.dot_general(
            eight, earlier, (((1,), (0,)), ((), ())), preferred_element_type=jnp.float32
        )[0:1]
        whole = lax.dot_general(
            eight, ones, (((1,), (0,)), ((), ())), preferred_element_type=jnp.float32
        )[0:1]
        rank = (below + seen).astype(jnp.int32)
        here = jnp.logical_and(mine, rank % n_member == me_group)
        spot[pl.ds(r, 1), :] = jnp.where(here, rank // n_member, -1)
        return seen + whole

    lax.fori_loop(0, n * per, count, jnp.zeros((1, LANES), jnp.float32))

    suffix = tail[...]
    upper = jnp.floor(suffix * (1.0 / LANES))
    table[...] = jnp.concatenate([upper, suffix - upper * LANES], axis=0).astype(jnp.bfloat16)
    bin_of = hi_of * LANES + lax.broadcasted_iota(jnp.int32, hi_of.shape, 1)
    kept = jnp.sum(
        jnp.sum(jnp.where(bin_of == cut[0], suffix, 0.0), axis=1, keepdims=True),
        axis=0, keepdims=True,
    )
    total = jnp.maximum(kept, 1.0)
    groups = weights.shape[0]
    group_of = lax.broadcasted_iota(jnp.int32, (groups, LANES), 0)
    weights[...] = jnp.zeros_like(weights)

    def weigh(r, c):
        bins = line(r, 0) // BIN_WIDTH
        slot = spot[pl.ds(r, 1), :]
        lo = jnp.where(lo_of == bins % LANES, 1.0, 0.0).astype(jnp.bfloat16)
        rows = lax.dot_general(
            table[...], lo, (((1,), (0,)), ((), ())), preferred_element_type=jnp.float32
        )
        pick = hi_of == bins // LANES
        up = jnp.sum(jnp.where(pick, rows[: BINS // LANES], 0.0), axis=0, keepdims=True)
        down = jnp.sum(jnp.where(pick, rows[BINS // LANES :], 0.0), axis=0, keepdims=True)
        at = jnp.logical_and(slot >= 0, group_of == slot // LANES)
        column = jnp.where(lo_of == slot % LANES, 1.0, 0.0).astype(jnp.bfloat16)
        both = jnp.concatenate([jnp.where(at, up, 0.0), jnp.where(at, down, 0.0)], axis=0)
        laid = lax.dot_general(
            both.astype(jnp.bfloat16), column, (((1,), (1,)), ((), ())),
            preferred_element_type=jnp.float32,
        )
        weights[...] += laid[:groups] * LANES + laid[groups:]
        return c

    lax.fori_loop(0, n * per, weigh, 0)
    weights[...] = weights[...] / total

    def done(rows, sem):
        rows = pl.ds(0, rows)
        pltpu.make_async_copy(send.at[rows], got.at[rows], sem).wait()

    done(w, own_sem)
    if spill:
        pltpu.make_async_copy(leaving.at[everything], joined.at[everything], leave_sem).wait()
    out = (n - len(wide) * n_member) * narrow + len(wide) * n_member * w
    if wide:
        def ends(size):
            done(out - size, send_sem)
            done((n - 1) * size, recv_sem)

        pl.when(is_wide(me))(functools.partial(ends, w))
        pl.when(jnp.logical_not(is_wide(me)))(functools.partial(ends, narrow))
    else:
        done(out - w, send_sem)
        done((n - 1) * w, recv_sem)


def pack_kernel(pieces, chunk, index, got, out, held, made, load_sem, out_sem):
    rows = got.shape[0]
    slots = made.shape[0]
    for k in range(8):
        part = pl.ds(k * (rows // 8), rows // 8)
        pltpu.make_async_copy(got.at[part], held.at[part], load_sem).start()
    load = pltpu.make_async_copy(got, held.at[pl.ds(0, rows)], load_sem)
    held[rows] = jnp.zeros(held.shape[1:], jnp.int32)
    load.wait()

    def stores(k):
        return [
            pltpu.make_async_copy(
                made.at[pl.ds(k * chunk, chunk), p, :],
                out.at[pl.ds(k * chunk, chunk), pl.ds(p * LANES, LANES)],
                out_sem.at[k, p],
            )
            for p in range(pieces)
        ]

    def fill(k):
        def some(g, c):
            for j in range(8):
                s = k * chunk + g * 8 + j
                made[s] = held[index[0, s]]
            return c

        lax.fori_loop(0, chunk // 8, some, 0)

    def step(k, c):
        fill(k)
        for copy in stores(k):
            copy.start()
        return c

    def finish(k, c):
        for copy in stores(k):
            copy.wait()
        return c

    lax.fori_loop(0, slots // chunk, step, 0)
    lax.fori_loop(0, slots // chunk, finish, 0)


def flows(views, w, w1):
    over = [jnp.maximum(v - w, 0) for v in views]
    free = [w - jnp.maximum(jnp.minimum(v, w), w1) for v in views]
    moved = []
    for step in (1, 2, 3):
        flow = [jnp.minimum(over[k], free[k ^ step]) for k in range(4)]
        over = [over[k] - flow[k] for k in range(4)]
        free = [free[k] - flow[k ^ step] for k in range(4)]
        moved.append(flow)
    return over[0], moved


def plan_kernel(
    n, n_member, slots, w1, caps, levels, cut, every, pairs, order,
    choice, index, spill_index, pick, rows_of,
):
    f32, i32, bf16 = jnp.float32, jnp.int32, jnp.bfloat16
    per = every.shape[1] // 2
    examples = per * LANES
    capacity = 2 * examples
    n_owner = n // n_member
    me_dp, me_group = lax.axis_index("dp"), lax.axis_index("group")
    me = me_dp * n_member + me_group

    def iota(shape, axis):
        return lax.broadcasted_iota(i32, shape, axis)

    def mm(a, b, dims=(((1,), (0,)), ((), ()))):
        return lax.dot_general(
            a.astype(bf16), b.astype(bf16), dims, preferred_element_type=f32
        )

    def one(flag):
        return jnp.where(flag, 1.0, 0.0)

    def rows(a):
        return jnp.sum(a, axis=0, keepdims=True)

    def lanes(a):
        return jnp.sum(a, axis=1, keepdims=True)

    side = ((((1,), (1,)), ((), ())))
    lane = iota((n, LANES), 1)
    home = lane // n_member
    member = lane % n_member
    src = iota((n, LANES), 0)
    small_r, small_c = iota((n, n), 0), iota((n, n), 1)

    kept = every[:, :per, :] // BIN_WIDTH >= cut[0]
    code = jnp.where(kept, every[:, per:, :], -1)
    table = jnp.zeros((n, LANES), f32)
    for o in range(n_owner):
        total = lanes(jnp.sum(one(code == o), axis=1))
        table = jnp.where(home == o, total, table)
    before = mm(one(small_c < small_r), table).astype(i32)
    skip = (member - before) & (n_member - 1)
    count = (table.astype(i32) - skip + n_member - 1) // n_member
    views = [count] + [
        mm(one(small_c == (small_r ^ k)), count.astype(f32)).astype(i32) for k in (1, 2, 3)
    ]

    sets = {}
    for width in sorted({w for level in levels for w in level}):
        left, moved = flows(views, width, w1)
        sets[width] = jnp.concatenate([left] + [moved[k][0] for k in range(3)], axis=0).astype(f32)
    col = iota((32, 4 * n), 1) // n
    limit = jnp.where(col == 0, 0.5, 0.0)
    for k, cap in enumerate(caps):
        limit = jnp.where(col == k + 1, cap + 0.5, limit)
    member_of = pairs[...]
    last = len(levels) * 28
    best = jnp.full((1, 1), last, i32)
    for number, (wide, narrow) in enumerate(levels):
        load = mm(member_of, sets[wide], side) + mm(1.0 - member_of, sets[narrow], side)
        bad = lanes(one(load > limit))
        rank = jnp.where(bad > 0.5, last, order[number][:, :1])
        best = jnp.minimum(best, jnp.min(rank, axis=0, keepdims=True))
    choice[...] = best
    w = jnp.zeros((1, LANES), f32)
    widest = jnp.zeros((1, 1), f32)
    for number, (wide, narrow) in enumerate(levels):
        hit = one(order[number] == best)
        found = rows(hit[:, :1])
        w = w + rows(hit * member_of) * (wide - narrow) + found * narrow
        widest = widest + found * wide
    w = jnp.where(best == last, float(slots), w).astype(i32)
    widest = jnp.where(best == last, float(slots), widest).astype(i32)
    _, moved = flows(views, w, w1)

    def row(a):
        return rows(jnp.where(src == me, a, 0))

    square_r, square_c = iota((LANES, LANES), 0), iota((LANES, LANES), 1)
    earlier = one(square_r < square_c)

    def running(a):
        return mm(jnp.broadcast_to(a.astype(f32), (8, LANES)), earlier)[:1].astype(i32)

    mine = every[me]
    my_code = jnp.where(mine[:per] // BIN_WIDTH >= cut[0], mine[per:], -1)
    owner_of = iota((n_owner, LANES), 0)
    seen = jnp.zeros((n_owner, 1), f32)
    found = jnp.zeros((LANES, LANES), i32)
    for r in range(per):
        line = my_code[r : r + 1]
        hot = one(owner_of == line)
        rank = rows(hot * (mm(hot, earlier) + seen)).astype(i32)
        rank = jnp.where(line >= 0, rank, -1)
        seen = seen + lanes(hot)
        at = one(square_r == rank)
        to = jnp.where(square_r // n_member == line, (square_c + 1).astype(f32), 0.0)
        got = mm(at, to, side).astype(i32)
        found = found + jnp.where(got > 0, got + r * LANES, 0)
    rows_of[...] = found

    own = jnp.minimum(row(views[0]), w)
    my_skip = row(skip)
    j = iota((slots, LANES), 0)
    local = jnp.zeros((slots, LANES), i32)
    for r in range(n_member):
        local = jnp.where(my_skip == r, rows_of[pl.ds(r, slots, stride=n_member), :], local)
    slot_row = jnp.where(j < own, jnp.maximum(local - 1, 0), 0)
    edge = jnp.maximum(own, w1)
    begin = own
    base = 0
    down = []
    inner = []
    for k, cap in enumerate(caps):
        coming, going = row(moved[k][k + 1]), row(moved[k][0])
        inside = (j >= edge) & (j < edge + coming)
        slot_row = jnp.where(inside, examples + base + running(coming) - edge + j, slot_row)
        edge = edge + coming
        lo = running(going)
        t = iota((cap, LANES), 0)
        inside = (t >= lo) & (t < lo + going)
        inner.append(one(inside))
        down.append(lanes(jnp.where(inside, my_skip + (begin - lo + t) * n_member + 1, 0)) - 1)
        begin = begin + going
        base += cap
    index[...] = slot_row
    inner = jnp.concatenate(inner, axis=0)
    down = jnp.concatenate(down, axis=0)
    room = sum(caps)
    hot = one(iota((room, LANES), 1) == down)
    high = found // LANES
    spread = mm(hot, high.astype(f32)) * LANES + mm(hot, (found - high * LANES).astype(f32))
    value = jnp.maximum(lanes(spread * inner) - 1.0, 0.0)
    turned = rows(jnp.where(iota((room, 256), 0) == iota((room, 256), 1), value, 0.0))
    spill_index[...] = turned.astype(i32)

    def column(a):
        return lanes(jnp.where(lane == me, a, 0))

    w_mine = lanes(jnp.where(lane[:1] == me, w, 0))
    owned = [jnp.minimum(column(v), w_mine) for v in views]
    source = iota((n, 1), 0)
    first = (column(before) - me_group + n_member - 1) // n_member
    near = jnp.minimum(owned[0], w1)
    block = n * w1 + source * (widest - w1) - w1
    spans = [(first, near, source * w1), (first + near, owned[0] - near, block + near)]
    at = first + owned[0]
    for k in range(len(caps)):
        going = column(moved[k][0])
        mate = k + 1
        slot = jnp.maximum(owned[mate], w1)
        for before_k in range(k):
            slot = slot + column(moved[before_k][mate ^ (before_k + 1)])
        spans.append((at, going, n * w1 + (source ^ mate) * (widest - w1) - w1 + slot))
        at = at + going
    t = iota((n, capacity), 1)
    where = jnp.zeros((n, capacity), i32)
    for lo, size, to in spans:
        where = where + jnp.where((t >= lo) & (t < lo + size), t + (to - lo + 1), 0)
    where = rows(where)
    pick[...] = jnp.where(where > 0, where - 1, capacity)


def body(n_owner, n_member, keys, cut, owner, tokens):
    examples, width = tokens.shape
    n = n_owner * n_member
    slots = 2 * examples // n
    capacity = 2 * examples
    pieces = width // LANES
    per = examples // LANES
    me_dp, me_group = lax.axis_index("dp"), lax.axis_index("group")
    me = me_dp * n_member + me_group
    vmem = pl.BlockSpec(memory_space=pltpu.VMEM)
    smem = pl.BlockSpec(memory_space=pltpu.SMEM)
    hbm = pl.BlockSpec(memory_space=pl.ANY)
    dest = owner[:, 0]
    i32 = jnp.int32

    mine = jnp.concatenate([keys.reshape(per, LANES), dest.reshape(per, LANES)], axis=0)
    every = pl.pallas_call(
        functools.partial(meta_kernel, n, n_member),
        out_shape=jax.ShapeDtypeStruct((n, 2 * per, LANES), jnp.int32),
        in_specs=[vmem],
        out_specs=vmem,
        scratch_shapes=[
            pltpu.SemaphoreType.DMA,
            pltpu.SemaphoreType.DMA,
            pltpu.SemaphoreType.DMA,
        ],
        compiler_params=pltpu.CompilerParams(collective_id=0, has_side_effects=True),
    )(mine)
    w1 = min(4, slots)
    variants = [((), slots, slots)]
    caps = ()
    if slots == 32 and n_owner == 8 and n_member == 4:
        caps = (96, 48, 24)
        found = []
        for w, narrow in LEVELS:
            for pair in itertools.combinations(range(n_owner), 2):
                size = [w if o in pair else narrow for o in range(n_owner)]
                half = n_owner // 2
                cost = max(sum(size[:half]), sum(size[half:]))
                found.append((cost, pair, w, narrow))
        variants = [f[1:] for f in sorted(found)] + variants
    room = sum(caps)
    sizes = np.array(
        [[w if o in pair else narrow for o in range(n_owner)] for pair, w, narrow in variants],
        np.int32,
    )
    if caps:
        order = np.full((len(LEVELS), 32, LANES), len(variants), np.int32)
        pairs = np.zeros((32, LANES), np.float32)
        for p, pair in enumerate(itertools.combinations(range(n_owner), 2)):
            for o in pair:
                pairs[p, o * n_member : (o + 1) * n_member] = 1
            for at, level in enumerate(LEVELS):
                order[at, p] = variants.index((pair,) + level)
        choice, index, spill_index, pick = pl.pallas_call(
            functools.partial(plan_kernel, n, n_member, slots, w1, caps, LEVELS),
            out_shape=(
                jax.ShapeDtypeStruct((1, 1), i32),
                jax.ShapeDtypeStruct((slots, LANES), i32),
                jax.ShapeDtypeStruct((1, 256), i32),
                jax.ShapeDtypeStruct((1, capacity), i32),
            ),
            in_specs=[smem, vmem, vmem, vmem],
            out_specs=(vmem,) * 4,
            scratch_shapes=[pltpu.VMEM((LANES, LANES), i32)],
        )(cut, every, jnp.asarray(pairs), jnp.asarray(order))
        choice = choice.reshape(())
    else:
        keys_all = every[:, :per].reshape(n * per, LANES)
        owner_all = every[:, per:].reshape(n * per, LANES)
        code_all = jnp.where(keys_all // BIN_WIDTH >= cut[0], owner_all, -1).reshape(n, examples)
        owners = jnp.arange(n_owner, dtype=i32)
        table = jnp.sum(code_all[:, None, :] == owners[None, :, None], axis=2, dtype=i32)
        source = jnp.arange(n, dtype=i32)
        before = jnp.sum(
            jnp.where((source[None, :] < source[:, None])[:, :, None], table[None], 0), axis=1
        )

        lane = np.arange(n)
        spread = (lane[None, :] // n_member == np.arange(n_owner)[:, None]).astype(np.float32)
        both = jnp.concatenate([table, before % n_member], axis=0).astype(jnp.float32)
        wide = jnp.dot(both, spread).astype(i32)
        member = jnp.arange(n, dtype=i32) % n_member
        skip = (member[None, :] - wide[n:] + n_member) % n_member
        count = jnp.maximum((wide[:n] - skip + n_member - 1) // n_member, 0)
        turn_of = np.concatenate(
            [lane[:, None] == (lane ^ k)[None, :] for k in range(4)], axis=0
        ).astype(np.float32)
        turned = jnp.dot(turn_of, count.astype(jnp.float32)).astype(i32)
        views = [turned[k * n : (k + 1) * n] for k in range(4)]
        skip_mine = jnp.sum(jnp.where((source == me)[:, None], skip, 0), axis=0)

        number = jnp.arange(len(variants), dtype=i32)
        choice = jnp.int32(0)
        picked = number[:, None] == choice
        w = jnp.sum(jnp.where(picked, np.repeat(sizes, n_member, axis=1), 0), axis=0)
        widest = jnp.max(w)
        _, moved = flows(views, w[None], w1)
        w_mine = jnp.sum(jnp.where(source == me, w, 0))

        here = source == me
        home = source // n_member

        def row(a):
            return jnp.sum(jnp.where(here[:, None], a, 0), axis=0)

        def running(a):
            return jnp.sum(jnp.where(source[None, :] < source[:, None], a[None, :], 0), axis=1)

        j = jnp.arange(slots, dtype=i32)[None, :]
        own = jnp.minimum(row(views[0]), w)
        first_of = home * capacity + skip_mine
        want = jnp.where(j < own[:, None], first_of[:, None] + j * n_member, -2)
        joins = jnp.zeros((n, slots), i32)
        leaves = []
        edge = jnp.maximum(own, w1)
        begin = own
        base = 0
        for k, cap in enumerate(caps):
            coming, going = row(moved[k][k + 1]), row(moved[k][0])
            inside = (j >= edge[:, None]) & (j < (edge + coming)[:, None])
            joins = jnp.where(inside, (examples + base + running(coming) - edge)[:, None] + j, joins)
            edge = edge + coming
            lo = running(going)
            t = jnp.arange(cap, dtype=i32)[:, None]
            inside = (t >= lo[None, :]) & (t < (lo + going)[None, :])
            at = (first_of + (begin - lo) * n_member)[None, :] + t * n_member + 1
            leaves.append(jnp.sum(jnp.where(inside, at, 0), axis=1) - 1)
            begin = begin + going
            base += cap
        want = jnp.concatenate([want.reshape(-1)] + leaves)

        code = jnp.where(keys // BIN_WIDTH >= cut[0], dest, -1)
        e = jnp.arange(examples, dtype=i32)
        local_rank = jnp.sum(
            (code[:, None] == code[None, :]) & (e[None, :] < e[:, None]), axis=1, dtype=i32
        )
        spot = jnp.where(code >= 0, code * capacity + local_rank, -9)
        match = jnp.sum(jnp.where(want[:, None] == spot[None, :], e[None, :], 0), axis=1)
        index = match[: n * slots] + joins.reshape(-1)
        spill_index = match[n * slots :] if caps else jnp.zeros((8,), i32)

        def column(a):
            return jnp.sum(jnp.where(here[None, :], a, 0), axis=1)

        mine_at = [column(v) for v in views]
        owned = [jnp.minimum(v, w_mine) for v in mine_at]
        first = jnp.sum(jnp.where(owners[None, :] == me_dp, before, 0), axis=1)
        first = (first - me_group + n_member - 1) // n_member
        near = jnp.minimum(owned[0], w1)
        block = n * w1 + source * (widest - w1) - w1
        spans = [(first, near, source * w1), (first + near, owned[0] - near, block + near)]
        at = first + owned[0]
        for k in range(len(caps)):
            going = column(moved[k][0])
            mate = k + 1
            slot = jnp.maximum(owned[mate], w1)
            for earlier in range(k):
                slot = slot + column(moved[earlier][mate ^ (earlier + 1)])
            there = jnp.bitwise_xor(source, mate)
            spans.append((at, going, n * w1 + there * (widest - w1) - w1 + slot))
            at = at + going
        lo = jnp.concatenate([s[0] for s in spans])
        size = jnp.concatenate([s[1] for s in spans])
        base = jnp.concatenate([s[2] for s in spans])
        t = jnp.arange(capacity, dtype=i32)[:, None]
        inside = (t >= lo[None, :]) & (t < (lo + size)[None, :])
        pick = jnp.sum(jnp.where(inside, t + (base - lo)[None, :] + 1, 0), axis=1)
        pick = jnp.where(pick > 0, pick - 1, capacity)
        index = index.reshape(n, slots).T
        spill_index, pick = spill_index[None], pick[None]

    def exchange(number):
        wide, w, narrow = variants[number]
        return pl.pallas_call(
            functools.partial(
                rows_kernel, n, n_member, slots, wide, w, narrow, w1, caps, pieces
            ),
            out_shape=(
                jax.ShapeDtypeStruct((capacity, pieces, LANES), jnp.int32),
                jax.ShapeDtypeStruct((BINS // LANES, LANES), jnp.int32),
                jax.ShapeDtypeStruct((capacity // LANES, LANES), jnp.float32),
            ),
            in_specs=[smem, smem, smem, hbm, vmem],
            out_specs=(hbm, vmem, vmem),
            scratch_shapes=[
                pltpu.VMEM((examples, pieces, LANES), jnp.int32),
                pltpu.VMEM((n * w, pieces, LANES), jnp.int32),
                pltpu.VMEM((max(room, 8), pieces, LANES), jnp.int32),
                pltpu.VMEM((max(room, 8), pieces, LANES), jnp.int32),
                pltpu.VMEM((n * per, LANES), jnp.int32),
                pltpu.VMEM((2 * BINS // LANES, LANES), jnp.bfloat16),
                pltpu.VMEM((BINS // LANES, LANES), jnp.float32),
            ]
            + [pltpu.SemaphoreType.DMA] * 6,
            compiler_params=pltpu.CompilerParams(
                collective_id=1 + number, has_side_effects=True,
                vmem_limit_bytes=60 * 1024 * 1024,
            ),
        )

    calls = [exchange(number) for number in range(len(variants))]
    choice, index, spill_index, pick = lax.optimization_barrier(
        (choice, index, spill_index, pick)
    )
    got, hist, weights = lax.switch(
        choice, calls, index, spill_index, cut, tokens, every
    )

    packed_rows = pl.pallas_call(
        functools.partial(pack_kernel, pieces, LANES),
        out_shape=jax.ShapeDtypeStruct((capacity, width), jnp.int32),
        in_specs=[smem, hbm],
        out_specs=hbm,
        scratch_shapes=[
            pltpu.VMEM((capacity + 1, pieces, LANES), jnp.int32),
            pltpu.VMEM((capacity, pieces, LANES), jnp.int32),
            pltpu.SemaphoreType.DMA,
            pltpu.SemaphoreType.DMA((capacity // LANES, pieces)),
        ],
        compiler_params=pltpu.CompilerParams(vmem_limit_bytes=60 * 1024 * 1024),
    )(pick, got)
    return (hist.reshape(BINS), packed_rows, weights.reshape(capacity))


def solution(mesh):
    placed = (P(("dp", "group")), P(), P(("dp", "group"), None), P(("dp", "group"), None))
    return jax.shard_map(
        functools.partial(body, mesh.shape["dp"], mesh.shape["group"]),
        mesh=mesh,
        in_specs=placed,
        out_specs=(P(), P(("dp", "group"), None), P(("dp", "group"))),
        check_vma=False,
    )
```
